32 devices in a mesh: dp: 16 (over z, x, core), tensor: 2 (over y).
Axes of the slice: x: 2, y: 2, z: 4, core: 2. Of those that a mesh axis runs over, the one named last changes fastest.
Arguments:
- tokens: bfloat16 [32768, 640], P(('dp', 'tensor')), may hold values from -6 to 6
- window_offsets: int32 [32], P('dp'), may hold values from 0 to 2047, as said below
- lengths: int32 [32], P('dp'), may hold values from 1 to 1024, as said below
- key_mask: int32 [32, 1024], P('dp'), may hold values from 0 to 1, as said below
- ln1_gain: float32 [640], replicated, may hold values from 0.5 to 1.5
- ln1_bias: float32 [640], replicated, may hold values from -1.5 to 1.5
- w_qkv: bfloat16 [3, 640, 640], P(None, None, 'tensor'), may hold values from -0.3125 to 0.3125
- qv_bias: float32 [2, 640], P(None, 'tensor'), may hold values from -1.5 to 1.5
- w_out: bfloat16 [640, 640], P('tensor'), may hold values from -1 to 1
- out_bias: float32 [640], replicated, may hold values from -1.5 to 1.5
- ln2_gain: float32 [640], replicated, may hold values from 0.5 to 1.5
- ln2_bias: float32 [640], replicated, may hold values from -1.5 to 1.5
- w_up: bfloat16 [640, 5120], P(None, 'tensor'), may hold values from -0.25 to 0.25
- up_bias: float32 [5120], P('tensor'), may hold values from -2.5 to 2.5
- w_down: bfloat16 [5120, 640], P('tensor'), may hold values from -0.15625 to 0.15625
- down_bias: float32 [640], replicated, may hold values from -1.5 to 1.5
- out_grad: bfloat16 [32768, 640], P(('dp', 'tensor')), may hold values from -6 to 6
Outputs:
- layer_out: bfloat16 [32768, 640], P(('dp', 'tensor'))
- tokens_grad: bfloat16 [32768, 640], P(('dp', 'tensor'))
- grad_ln1_gain: float32 [640], replicated
- grad_ln1_bias: float32 [640], replicated
- grad_w_qkv: float32 [3, 640, 640], P(None, None, 'tensor')
- grad_qv_bias: float32 [2, 640], P(None, 'tensor')
- grad_w_out: float32 [640, 640], P('tensor')
- grad_out_bias: float32 [640], replicated
- grad_ln2_gain: float32 [640], replicated
- grad_ln2_bias: float32 [640], replicated
- grad_w_up: float32 [640, 5120], P(None, 'tensor')
- grad_up_bias: float32 [5120], P('tensor')
- grad_w_down: float32 [5120, 640], P('tensor')
- grad_down_bias: float32 [640], replicated
The draws below stay inside these ranges and needn't reach their ends.
Inputs may be any that keep to these rules, and one draw needn't show every extreme that they name: `window_offsets`: rows 2i and 2i+1 form pair i. Either both offsets are 0, or the second exceeds the first by 512 to 1024. Rows 0 and 1 are of the second kind, with offsets 1024 - 1 and 2047; rows 2 and 3 are of the first kind. `lengths`: both rows of a pair whose second offset exceeds its first have length 1024. key_mask[r, 0] is 1 for every row r.
All inputs are finite; a program needn't handle non-finite values.
Results may differ from the reference program's by a relative error of at most 0.014.
The reference program's roundings to bfloat16 on the way count: a program that leaves them out, or rounds other values in their place, can miss the bound.
Values may be sent and summed in bfloat16 or wider, within the bound.
A program may use at most 320 MiB of HBM per device.

```python
import math
from functools import partial
import jax
import jax.numpy as jnp
from jax import lax

D = 640
HEADS = 20
HEAD = 32
FF = 5120
SEQ = 1024
PAIRS = 16
ROWS = 32
TOKENS = 32768


def pair_layout(key):
    base_key = jax.random.fold_in(key, 11)
    kind_key, start_key, shift_key, length_key = jax.random.split(base_key, 4)
    joined = jax.random.randint(kind_key, (PAIRS,), 0, 2)
    joined = joined.at[0].set(1).at[1].set(0)
    start_pos = jax.random.randint(start_key, (PAIRS,), 0, SEQ)
    start_pos = start_pos.at[0].set(SEQ - 1)
    shift_by = jax.random.randint(shift_key, (PAIRS,), SEQ // 2, SEQ + 1)
    shift_by = shift_by.at[0].set(SEQ)
    short_len = jax.random.randint(length_key, (PAIRS, 2), 1, SEQ + 1)
    offsets = jnp.where(joined[:, None] == 1, jnp.stack([start_pos, start_pos + shift_by], axis=1), 0)
    item_lengths = jnp.where(joined[:, None] == 1, SEQ, short_len)
    return (offsets.reshape(ROWS).astype(jnp.int32), item_lengths.reshape(ROWS).astype(jnp.int32))


def draw_window_offsets(key, part):
    return pair_layout(key)[0]


def draw_lengths(key, part):
    return pair_layout(key)[1]


def draw_key_mask(key, part):
    mask_draw = jax.random.randint(jax.random.fold_in(key, 23), (ROWS, SEQ), 0, 8)
    first_col = lax.broadcasted_iota(jnp.int32, (ROWS, SEQ), 1) == 0
    mask_draw = jnp.where(first_col, 1, mask_draw)
    return (mask_draw > 0).astype(jnp.int32)


def shard_levels(rng, dims, cuts, least, high):
    loudness, own = 1.0, jax.random.fold_in(rng, 6)
    for axis_at, shards_of in cuts:
        draws = jnp.exp(jax.random.uniform(jax.random.fold_in(own, axis_at), (shards_of,), jnp.float32, least / len(cuts), high / len(cuts)))
        loudness = loudness * jnp.repeat(draws, dims[axis_at] // shards_of).reshape([-1 if axis == axis_at else 1 for axis in range(len(dims))])
    return loudness


def noise(rng, dims, scale, most, shards=(), held_as=jnp.bfloat16):
    result = scale * jax.random.normal(rng, dims, jnp.float32)
    if shards:
        result = result * shard_levels(rng, dims, shards, -0.22, 0.18)
    return jnp.clip(result, -most, most).astype(held_as)


def setup_inputs(seed: int = 0) -> dict:
    keys = jax.random.split(jax.random.key(seed), 18)
    return {
        "tokens": noise(keys[0], (TOKENS, D), 1.0, 6.0, ((0, 32),)),
        "window_offsets": draw_window_offsets(jax.random.fold_in(keys[17], 71), 0),
        "lengths": draw_lengths(jax.random.fold_in(keys[17], 71), 0),
        "key_mask": draw_key_mask(jax.random.fold_in(keys[17], 71), 0),
        "ln1_gain": jnp.clip(1.0 + 0.1 * jax.random.normal(keys[4], (D,), jnp.float32), 0.5, 1.5),
        "ln1_bias": noise(keys[5], (D,), 0.3, 1.5, (), jnp.float32),
        "w_qkv": noise(keys[6], (3, D, D), (D // 2) ** -0.5, 0.3125, ((2, 2),)),
        "qv_bias": noise(keys[7], (2, D), 0.3, 1.5, ((1, 2),), jnp.float32),
        "w_out": noise(keys[8], (D, D), (D // 16) ** -0.5, 1.0, ((0, 2),)),
        "out_bias": noise(keys[9], (D,), 0.3, 1.5, (), jnp.float32),
        "ln2_gain": jnp.clip(1.0 + 0.1 * jax.random.normal(keys[10], (D,), jnp.float32), 0.5, 1.5),
        "ln2_bias": noise(keys[11], (D,), 0.3, 1.5, (), jnp.float32),
        "w_up": noise(keys[12], (D, FF), D ** -0.5, 0.25, ((1, 2),)),
        "up_bias": noise(keys[13], (FF,), 0.5, 2.5, ((0, 2),), jnp.float32),
        "w_down": noise(keys[14], (FF, D), (FF // 4) ** -0.5, 0.15625, ((0, 2),)),
        "down_bias": noise(keys[15], (D,), 0.3, 1.5, (), jnp.float32),
        "out_grad": noise(keys[16], (TOKENS, D), 1.0, 6.0, ((0, 32),)),
    }


@jax.custom_vjp
def low(v):
    return lax.optimization_barrier(v.astype(jnp.bfloat16)).astype(jnp.float32)

@jax.custom_vjp
def low_back(v):
    return v

def low_keep(v):
    return (low(v), None)

def low_pass(kept, grad):
    return (grad,)

def back_keep(v):
    return (v, None)

def back_low(kept, grad):
    return (low(grad),)
low.defvjp(low_keep, low_pass)
low_back.defvjp(back_keep, back_low)
epsilon = 1e-05
masked_score = -1000000000.0

def layer_norm(inputs, gain_vec, bias_vec):
    center = inputs - lax.optimization_barrier(jnp.mean(inputs, axis=-1, keepdims=True))
    spread = lax.optimization_barrier(jnp.mean(center * center, axis=-1, keepdims=True))
    return center * lax.rsqrt(spread + epsilon) * gain_vec + bias_vec

def pair_keys(offsets, item_lengths, key_flags):
    seq_len = key_flags.shape[1]
    column = lax.broadcasted_iota(jnp.int32, (2, seq_len), 1)
    second = lax.broadcasted_iota(jnp.int32, (2, seq_len), 0) == 1
    joined = offsets[1] > offsets[0]
    repeat = second & joined & (offsets[1] + column < offsets[0] + seq_len)
    live_keys = (key_flags == 1) & (column < item_lengths[:, None]) & jnp.logical_not(repeat)
    return (live_keys.reshape(2 * seq_len), joined)

def allowed_block(live_keys, joined, first_row, row_count, seq_len):
    query_row = (first_row + lax.iota(jnp.int32, row_count)) // seq_len
    key_row = lax.iota(jnp.int32, 2 * seq_len) // seq_len
    return live_keys[None, :] & (joined | (query_row[:, None] == key_row[None, :]))

def attend_pair(query_pair, key_pair, value_pair, live_keys, joined):
    pair_span = query_pair.shape[0]
    highest = lax.Precision.HIGHEST
    scores = jnp.einsum('qhe,khe->hqk', query_pair, key_pair, precision=highest) * (1.0 / math.sqrt(HEAD))
    scores = low_back(scores)
    allowed = allowed_block(live_keys, joined, 0, pair_span, pair_span // 2)
    scores = jnp.where(allowed[None], scores, masked_score)
    row_max = lax.optimization_barrier(jnp.max(scores, axis=-1, keepdims=True))
    exponent = jnp.exp(scores - row_max)
    prob_low = low(exponent / lax.optimization_barrier(jnp.sum(exponent, axis=-1, keepdims=True)))
    mixed_heads = jnp.einsum('hqk,khe->qhe', prob_low, value_pair, precision=highest)
    return mixed_heads.reshape(pair_span, HEADS * HEAD)

def one_pair(carry_in, pair_items):
    query_pair, key_pair, value_pair, live_pair, joined_pair = pair_items
    return (carry_in, attend_pair(query_pair, key_pair, value_pair, live_pair, joined_pair))

def forward(tokens_f, params, live_all, joined_all):
    ln1_gain, ln1_bias, w_qkv, qv_bias, w_out, out_bias, ln2_gain, ln2_bias, w_up, up_bias, w_down, down_bias = params
    highest = lax.Precision.HIGHEST
    normed = low(layer_norm(tokens_f, ln1_gain, ln1_bias))
    projected = jnp.einsum('td,cde->tce', normed, w_qkv, precision=highest)
    query_tok = low(low_back(projected[:, 0] + qv_bias[0]))
    key_tok = low(low_back(projected[:, 1]))
    value_tok = low(low_back(projected[:, 2] + qv_bias[1]))
    shaped = (PAIRS, 2 * SEQ, HEADS, HEAD)
    step_fn = jax.checkpoint(one_pair)
    _, mixed_heads = lax.scan(step_fn, jnp.zeros((), jnp.float32), (query_tok.reshape(shaped), key_tok.reshape(shaped), value_tok.reshape(shaped), live_all, joined_all))
    heads_out = low(low_back(mixed_heads.reshape(TOKENS, D)))
    attn_out = low_back(jnp.dot(heads_out, w_out, precision=highest) + out_bias)
    residual_mid = tokens_f + attn_out
    normed_mid = low(layer_norm(residual_mid, ln2_gain, ln2_bias))
    upper = low_back(jnp.dot(normed_mid, w_up, precision=highest) + up_bias)
    activated = low(jax.nn.gelu(upper, approximate=False))
    branch = low_back(jnp.dot(activated, w_down, precision=highest) + down_bias)
    return residual_mid + branch

def reference(tokens, window_offsets, lengths, key_mask, ln1_gain, ln1_bias, w_qkv, qv_bias, w_out, out_bias, ln2_gain, ln2_bias, w_up, up_bias, w_down, down_bias, out_grad):
    live_all, joined_all = jax.vmap(pair_keys)(window_offsets.reshape(PAIRS, 2), lengths.reshape(PAIRS, 2), key_mask.reshape(PAIRS, 2, SEQ))
    params = tuple((param_entry.astype(jnp.float32) for param_entry in (ln1_gain, ln1_bias, w_qkv, qv_bias, w_out, out_bias, ln2_gain, ln2_bias, w_up, up_bias, w_down, down_bias)))
    tokens_f = tokens.astype(jnp.float32)
    layer_fn = partial(forward, live_all=live_all, joined_all=joined_all)
    out_f, pullback = jax.vjp(layer_fn, tokens_f, params)
    grad_tok, grad_par = pullback(out_grad.astype(jnp.float32))
    return (out_f.astype(jnp.bfloat16), grad_tok.astype(jnp.bfloat16), grad_par[0], grad_par[1], grad_par[2], grad_par[3], grad_par[4], grad_par[5], grad_par[6], grad_par[7], grad_par[8], grad_par[9], grad_par[10], grad_par[11])
```

```python
import math
import functools
import jax
import jax.numpy as jnp
from jax import lax
from jax.experimental import pallas as pl
from jax.experimental.pallas import tpu as pltpu
from jax.sharding import PartitionSpec as P

HEAD = 32
LOG2E = 1.0 / math.log(2.0)
F32, BF16 = jnp.float32, jnp.bfloat16


def three_terms(x):
    a = x.astype(BF16)
    r = x - a.astype(F32)
    b = r.astype(BF16)
    c = (r - b.astype(F32)).astype(BF16)
    return a, b, c


def scaled_pair(q_t):
    q_s = q_t.astype(F32) * (LOG2E / math.sqrt(HEAD))
    hi = q_s.astype(BF16)
    return hi, (q_s - hi.astype(F32)).astype(BF16)


def rows16(parts, width):
    row = lax.broadcasted_iota(jnp.int32, (16, width), 0)
    out = jnp.zeros((16, width), F32)
    for i, part in enumerate(parts):
        out = jnp.where(row == i, part, out)
    return out.astype(BF16)


def key_rows(k_t, bias):
    keys = k_t.shape[1]
    aux = rows16([bias, -1.0, -1.0, -1.0], keys)
    pad = jnp.zeros((48, keys), BF16)
    return jnp.concatenate([k_t, k_t, aux, pad], axis=0).T


def fwd_kernel(heads, q_block, chunk, q_ref, k_ref, v_ref, bias_ref, o_ref, l_ref, k_aug, s_a, s_b):
    queries, keys = q_ref.shape[1], k_ref.shape[1]
    steps = [(h, b) for h in range(heads) for b in range(queries // q_block)]
    slots = (s_a, s_b)
    ones = rows16([1.0], keys)

    def scores(step):
        h, b = steps[step]
        slot = slots[step % 2]
        rows = slice(h * HEAD, (h + 1) * HEAD)
        if b == 0:
            k_aug[h % 2] = key_rows(k_ref[rows, :], bias_ref[...])
        hi, lo = scaled_pair(q_ref[rows, b * q_block:(b + 1) * q_block])
        q_aug = jnp.concatenate(
            [hi, lo, rows16([1.0], q_block), jnp.zeros((48, q_block), BF16)], axis=0)
        top = None
        for c in range(keys // chunk):
            s = jnp.dot(k_aug[h % 2, c * chunk:(c + 1) * chunk, :], q_aug, preferred_element_type=F32)
            slot[c * chunk:(c + 1) * chunk, :] = s
            m = jnp.max(s, axis=0, keepdims=True)
            top = m if top is None else jnp.maximum(top, m)
        return top

    def mix(step, top):
        h, b = steps[step]
        slot = slots[step % 2]
        rows = slice(h * HEAD, (h + 1) * HEAD)
        cols = slice(b * q_block, (b + 1) * q_block)
        v_aug = jnp.concatenate([v_ref[rows, :], ones], axis=0)
        acc = jnp.zeros((48, q_block), F32)
        for c in range(keys // chunk):
            p = jnp.exp2(slot[c * chunk:(c + 1) * chunk, :] - top).astype(BF16)
            acc = acc + jnp.dot(v_aug[:, c * chunk:(c + 1) * chunk], p, preferred_element_type=F32)
        total = acc[HEAD:HEAD + 1, :]
        o_ref[rows, cols] = (acc[:HEAD] * (1.0 / total)).astype(BF16)
        l_ref[0, h:h + 1, cols] = top + jnp.log2(total)

    top = scores(0)
    for step in range(len(steps)):
        after = scores(step + 1) if step + 1 < len(steps) else None
        mix(step, top)
        top = after


def attention_forward(q_t, k_t, v_t, bias, heads=2, q_block=256, chunk=512):
    width, queries = q_t.shape
    keys = k_t.shape[1]
    all_heads = width // HEAD
    rows = heads * HEAD
    return pl.pallas_call(
        functools.partial(fwd_kernel, heads, q_block, chunk),
        name="attn_fwd",
        grid=(all_heads // heads,),
        out_shape=(jax.ShapeDtypeStruct((width, queries), BF16),
                   jax.ShapeDtypeStruct((all_heads // heads, heads, queries), F32)),
        in_specs=[pl.BlockSpec((rows, queries), lambda i: (i, 0)),
                  pl.BlockSpec((rows, keys), lambda i: (i, 0)),
                  pl.BlockSpec((rows, keys), lambda i: (i, 0)),
                  pl.BlockSpec((1, keys), lambda i: (0, 0))],
        out_specs=(pl.BlockSpec((rows, queries), lambda i: (i, 0)),
                   pl.BlockSpec((1, heads, queries), lambda i: (i, 0, 0))),
        scratch_shapes=[pltpu.VMEM((2, keys, 128), BF16),
                        pltpu.VMEM((keys, q_block), F32),
                        pltpu.VMEM((keys, q_block), F32)],
        compiler_params=pltpu.CompilerParams(vmem_limit_bytes=56 << 20),
        cost_estimate=pl.CostEstimate(
            flops=16 * 2 * HEAD * 2 * all_heads * queries * keys,
            transcendentals=all_heads * queries * keys,
            bytes_accessed=4 * width * keys * 2),
    )(q_t, k_t, v_t, bias)


def bwd_kernel(heads, q_block, chunk, form, q_ref, k_ref, v_ref, bias_ref, o_ref, g_ref, l_ref,
               dq_ref, dk_ref, dv_ref, k_aug, v_aug, dk_acc, dv_acc):
    queries, keys = q_ref.shape[1], k_ref.shape[1]
    scale = 1.0 / math.sqrt(HEAD)
    for h in range(heads):
        rows = slice(h * HEAD, (h + 1) * HEAD)
        k_t = k_ref[rows, :]
        k_aug[...] = key_rows(k_t, bias_ref[...])
        minus = rows16([-1.0, -1.0, -1.0], keys)
        v_aug[...] = jnp.concatenate(
            [v_ref[rows, :], minus, jnp.zeros((80, keys), BF16)], axis=0).T
        for b in range(queries // q_block):
            cols = slice(b * q_block, (b + 1) * q_block)
            q_t = q_ref[rows, cols]
            g_t = g_ref[rows, cols]
            hi, lo = scaled_pair(q_t)
            l3 = three_terms(l_ref[0, h:h + 1, cols])
            q_aug = jnp.concatenate(
                [hi, lo, rows16([1.0] + [t.astype(F32) for t in l3], q_block),
                 jnp.zeros((48, q_block), BF16)], axis=0)
            inner = jnp.sum(g_t.astype(F32) * o_ref[rows, cols].astype(F32), axis=0, keepdims=True)
            g_aug = jnp.concatenate(
                [g_t, rows16([t.astype(F32) for t in three_terms(inner)], q_block),
                 jnp.zeros((80, q_block), BF16)], axis=0)
            if form == "stream":
                q_n, g_n = q_t.T, g_t.T
            dq = jnp.zeros((HEAD, q_block), F32)
            for c in range(keys // chunk):
                span = slice(c * chunk, (c + 1) * chunk)
                p = jnp.exp2(jnp.dot(k_aug[span, :], q_aug, preferred_element_type=F32))
                d = p * jnp.dot(v_aug[span, :], g_aug, preferred_element_type=F32)
                p, d = p.astype(BF16), d.astype(BF16)
                if form == "stream":
                    dv = jnp.dot(p, g_n, preferred_element_type=F32)
                    dk = jnp.dot(d, q_n, preferred_element_type=F32)
                    if b == 0:
                        dv_acc[span, :] = dv
                        dk_acc[span, :] = dk
                    else:
                        dv_acc[span, :] += dv
                        dk_acc[span, :] += dk
                else:
                    nt = (((1,), (1,)), ((), ()))
                    dv = lax.dot_general(g_t, p, nt, preferred_element_type=F32)
                    dk = lax.dot_general(q_t, d, nt, preferred_element_type=F32)
                    if b == 0:
                        dv_acc[:, span] = dv
                        dk_acc[:, span] = dk
                    else:
                        dv_acc[:, span] += dv
                        dk_acc[:, span] += dk
                dq = dq + jnp.dot(k_t[:, span], d, preferred_element_type=F32)
            dq_ref[rows, cols] = (dq * scale).astype(BF16)
        if form == "stream":
            dv_ref[rows, :] = dv_acc[...].T.astype(BF16)
            dk_ref[rows, :] = (dk_acc[...].T * scale).astype(BF16)
        else:
            dv_ref[rows, :] = dv_acc[...].astype(BF16)
            dk_ref[rows, :] = (dk_acc[...] * scale).astype(BF16)


def attention_backward(q_t, k_t, v_t, bias, o_t, g_t, lse, heads=2, q_block=512, chunk=512,
                       form="nt", first=0, count=None):
    width, queries = q_t.shape
    keys = k_t.shape[1]
    rows = heads * HEAD
    count = width // rows if count is None else count
    some = lambda i: (i + first, 0)
    acc = (keys, HEAD) if form == "stream" else (HEAD, keys)
    q_spec = pl.BlockSpec((rows, queries), some)
    k_spec = pl.BlockSpec((rows, keys), some)
    out = lambda i: (i, 0)
    return pl.pallas_call(
        functools.partial(bwd_kernel, heads, q_block, chunk, form),
        name="attn_bwd",
        grid=(count,),
        out_shape=(jax.ShapeDtypeStruct((count * rows, queries), BF16),
                   jax.ShapeDtypeStruct((count * rows, keys), BF16),
                   jax.ShapeDtypeStruct((count * rows, keys), BF16)),
        in_specs=[q_spec, k_spec, k_spec, pl.BlockSpec((1, keys), lambda i: (0, 0)), q_spec, q_spec,
                  pl.BlockSpec((1, heads, queries), lambda i: (i + first, 0, 0))],
        out_specs=(pl.BlockSpec((rows, queries), out), pl.BlockSpec((rows, keys), out),
                   pl.BlockSpec((rows, keys), out)),
        scratch_shapes=[pltpu.VMEM((keys, 128), BF16), pltpu.VMEM((keys, 128), BF16),
                        pltpu.VMEM(acc, F32), pltpu.VMEM(acc, F32)],
        compiler_params=pltpu.CompilerParams(vmem_limit_bytes=56 << 20),
        cost_estimate=pl.CostEstimate(
            flops=16 * 5 * HEAD * 2 * count * heads * queries * keys // 2,
            transcendentals=count * heads * queries * keys,
            bytes_accessed=count * rows * (3 * queries + 4 * keys) * 2),
    )(q_t, k_t, v_t, bias, o_t, g_t, lse)

epsilon = 1e-05
masked_score = -1000000000.0


def layer_norm(inputs, gain_vec, bias_vec):
    center = inputs - jnp.mean(inputs, axis=-1, keepdims=True)
    spread = jnp.mean(center * center, axis=-1, keepdims=True)
    return center * lax.rsqrt(spread + epsilon) * gain_vec + bias_vec


def gelu_exact(inputs):
    return jax.nn.gelu(inputs, approximate=False)


def pair_keys(offsets, item_lengths, key_flags):
    seq_len = key_flags.shape[1]
    column = lax.broadcasted_iota(jnp.int32, (2, seq_len), 1)
    second = lax.broadcasted_iota(jnp.int32, (2, seq_len), 0) == 1
    joined = offsets[1] > offsets[0]
    repeat = second & joined & (offsets[1] + column < offsets[0] + seq_len)
    live_keys = (key_flags == 1) & (column < item_lengths[:, None]) & jnp.logical_not(repeat)
    return live_keys, joined


def einsum32(spec, a, b):
    return jnp.einsum(spec, a, b, preferred_element_type=F32)


def body(
    dp_count,
    tokens,
    window_offsets,
    lengths,
    key_mask,
    ln1_gain,
    ln1_bias,
    w_qkv,
    qv_bias,
    w_out,
    out_bias,
    ln2_gain,
    ln2_bias,
    w_up,
    up_bias,
    w_down,
    down_bias,
    out_grad,
):
    side = lax.axis_index("tensor")
    core = lax.axis_index("dp") % 2
    core_groups = [list(range(c, dp_count, 2)) for c in range(2)]

    def swap_side(x):
        return lax.ppermute(x, "tensor", [(0, 1), (1, 0)])

    def swap_core(x):
        return lax.ppermute(x, "dp", [(i, i ^ 1) for i in range(dp_count)])

    def halves(x, axis):
        size = x.shape[axis] // 2
        return (lax.dynamic_slice_in_dim(x, core * size, size, axis),
                lax.dynamic_slice_in_dim(x, (1 - core) * size, size, axis))

    def ordered(first, second, flag, axis):
        return jnp.where(flag == 0, jnp.concatenate([first, second], axis),
                         jnp.concatenate([second, first], axis))

    def whole(shard, axis):
        near, far = halves(shard, axis)
        other_near = swap_side(near)
        return jnp.concatenate([near, far, other_near, swap_core(other_near)], axis)

    def reduced(grad, axis):
        size = grad.shape[axis] // 4
        near, far, other_near, other_far = (
            lax.slice_in_dim(grad, i * size, (i + 1) * size, axis=axis) for i in range(4))
        got = swap_core(jnp.concatenate([far, other_far], axis).astype(BF16))
        got_own, got_other = jnp.split(got, 2, axis)
        across = swap_side((other_near + got_other.astype(F32)).astype(BF16))
        mine = (near + got_own.astype(F32) + across.astype(F32)).astype(BF16)
        mine = lax.psum(mine, "dp", axis_index_groups=core_groups)
        return ordered(mine, swap_core(mine), core, axis).astype(F32)

    w_qkv_all = whole(w_qkv, 2)
    tokens_other = swap_side(tokens)
    biases = jnp.concatenate([qv_bias.reshape(-1), up_bias])
    biases_other = swap_side(biases)
    local = qv_bias.shape[1]

    def local_order(own, other):
        return jnp.concatenate(halves(own, own.ndim - 1) + halves(other, other.ndim - 1), axis=-1)

    qv_all = local_order(qv_bias, biases_other[:2 * local].reshape(2, local))
    up_bias_all = local_order(up_bias, biases_other[2 * local:])
    w_out_all = whole(w_out, 0)
    w_up_all = whole(w_up, 1)
    w_down_all = whole(w_down, 0)

    live, joined = pair_keys(window_offsets, lengths, key_mask)
    live_own = lax.dynamic_index_in_dim(live, side, 0, keepdims=False)
    live_other = lax.dynamic_index_in_dim(live, 1 - side, 0, keepdims=False) & joined
    bias = jnp.where(jnp.concatenate([live_own, live_other]), 0.0, masked_score)[None].astype(F32)

    tokens_f = tokens.astype(F32)
    normed = layer_norm(tokens_f, ln1_gain, ln1_bias).astype(BF16)
    normed_other = layer_norm(tokens_other.astype(F32), ln1_gain, ln1_bias).astype(BF16)
    normed_both = jnp.concatenate([normed, normed_other], axis=0)
    query = (einsum32("td,de->et", normed, w_qkv_all[0]) + qv_all[0][:, None]).astype(BF16)
    key = einsum32("td,de->et", normed_both, w_qkv_all[1]).astype(BF16)
    value = (einsum32("td,de->et", normed_both, w_qkv_all[2]) + qv_all[1][:, None]).astype(BF16)
    heads_out, log_norm = attention_forward(query, key, value, bias)

    residual_mid = tokens_f + (einsum32("et,ed->td", heads_out, w_out_all) + out_bias)
    normed_mid = layer_norm(residual_mid, ln2_gain, ln2_bias).astype(BF16)
    upper = jnp.dot(normed_mid, w_up_all, preferred_element_type=F32) + up_bias_all
    activated = gelu_exact(upper).astype(BF16)
    branch = jnp.dot(activated, w_down_all, preferred_element_type=F32) + down_bias
    layer_out = (residual_mid + branch).astype(BF16)

    grad_w_down = einsum32("tf,td->fd", activated, out_grad)
    grad_w_down = reduced(grad_w_down, 0)
    grad_act = einsum32("td,fd->tf", out_grad, w_down_all)
    _, gelu_back = jax.vjp(gelu_exact, upper)
    grad_upper = gelu_back(grad_act)[0].astype(BF16)
    grad_w_up = reduced(einsum32("td,tf->df", normed_mid, grad_upper), 1)
    grad_up_bias = jnp.sum(grad_upper, axis=0, dtype=F32)
    grad_normed_mid = einsum32("tf,df->td", grad_upper, w_up_all)
    _, norm2_back = jax.vjp(layer_norm, residual_mid, ln2_gain, ln2_bias)
    grad_mid_part, grad_ln2_gain, grad_ln2_bias = norm2_back(grad_normed_mid)
    grad_mid = out_grad.astype(F32) + grad_mid_part
    grad_mid_low = grad_mid.astype(BF16)
    grad_w_out = reduced(einsum32("et,td->ed", heads_out, grad_mid_low), 0)
    grad_heads = einsum32("td,ed->et", grad_mid_low, w_out_all).astype(BF16)
    grad_query, grad_key, grad_value = attention_backward(
        query, key, value, bias, heads_out, grad_heads, log_norm)

    seq_len = tokens.shape[0]
    grad_normed_kv = (einsum32("et,de->td", grad_key, w_qkv_all[1])
                      + einsum32("et,de->td", grad_value, w_qkv_all[2]))
    from_other = swap_side(grad_normed_kv[seq_len:].astype(BF16))
    grad_w_qkv = reduced(jnp.stack([
        einsum32("td,et->de", normed, grad_query),
        einsum32("td,et->de", normed_both, grad_key),
        einsum32("td,et->de", normed_both, grad_value)]), 2)
    grad_qv_bias = jnp.stack([jnp.sum(grad_query, axis=1, dtype=F32),
                              jnp.sum(grad_value, axis=1, dtype=F32)])
    grad_normed = (grad_normed_kv[:seq_len] + einsum32("et,de->td", grad_query, w_qkv_all[0])
                   + from_other.astype(F32))
    _, norm1_back = jax.vjp(layer_norm, tokens_f, ln1_gain, ln1_bias)
    grad_tok_part, grad_ln1_gain, grad_ln1_bias = norm1_back(grad_normed)
    tokens_grad = (grad_mid + grad_tok_part).astype(BF16)
    grad_out_bias = jnp.sum(grad_mid_low, axis=0, dtype=F32)
    grad_down_bias = jnp.sum(out_grad, axis=0, dtype=F32)

    def global_order(x):
        near, far, other_near, other_far = jnp.split(x, 4, axis=-1)
        return ordered(ordered(near, far, core, -1), ordered(other_near, other_far, core, -1), side, -1)

    smalls = [grad_ln1_gain, grad_ln1_bias, grad_ln2_gain, grad_ln2_bias, grad_out_bias,
              grad_down_bias, global_order(grad_qv_bias).reshape(-1), global_order(grad_up_bias)]
    packed = lax.psum(jnp.concatenate(smalls), ("dp", "tensor"))
    width = ln1_gain.shape[0]
    vectors = [packed[i * width:(i + 1) * width] for i in range(6)]
    at = 6 * width
    qv_sum = packed[at:at + 4 * local].reshape(2, 2 * local)
    up_sum = packed[at + 4 * local:]
    grad_qv_bias = lax.dynamic_slice_in_dim(qv_sum, side * local, local, 1)
    grad_up_bias = lax.dynamic_slice_in_dim(up_sum, side * up_bias.shape[0], up_bias.shape[0], 0)
    return (
        layer_out,
        tokens_grad,
        vectors[0],
        vectors[1],
        grad_w_qkv,
        grad_qv_bias,
        grad_w_out,
        vectors[4],
        vectors[2],
        vectors[3],
        grad_w_up,
        grad_up_bias,
        grad_w_down,
        vectors[5],
    )


def solution(mesh):
    in_specs = (
        P(("dp", "tensor"), None),
        P("dp"),
        P("dp"),
        P("dp", None),
        P(),
        P(),
        P(None, None, "tensor"),
        P(None, "tensor"),
        P("tensor", None),
        P(),
        P(),
        P(),
        P(None, "tensor"),
        P("tensor"),
        P("tensor", None),
        P(),
        P(("dp", "tensor"), None),
    )
    out_specs = (
        P(("dp", "tensor"), None),
        P(("dp", "tensor"), None),
        P(),
        P(),
        P(None, None, "tensor"),
        P(None, "tensor"),
        P("tensor", None),
        P(),
        P(),
        P(),
        P(None, "tensor"),
        P("tensor"),
        P("tensor", None),
        P(),
    )
    bound = functools.partial(body, mesh.shape["dp"])
    return jax.shard_map(bound, mesh=mesh, in_specs=in_specs, out_specs=out_specs, check_vma=False)
```

```python
import math
import functools
import jax
import jax.numpy as jnp
from jax import lax
from jax.experimental import pallas as pl
from jax.experimental.pallas import tpu as pltpu
from jax.sharding import PartitionSpec as P

HEAD = 32
LOG2E = 1.0 / math.log(2.0)
F32, BF16 = jnp.float32, jnp.bfloat16


def three_terms(x):
    a = x.astype(BF16)
    r = x - a.astype(F32)
    b = r.astype(BF16)
    c = (r - b.astype(F32)).astype(BF16)
    return a, b, c


def scaled_pair(q_t):
    q_s = q_t.astype(F32) * (LOG2E / math.sqrt(HEAD))
    hi = q_s.astype(BF16)
    return hi, (q_s - hi.astype(F32)).astype(BF16)


def rows16(parts, width):
    row = lax.broadcasted_iota(jnp.int32, (16, width), 0)
    out = jnp.zeros((16, width), F32)
    for i, part in enumerate(parts):
        out = jnp.where(row == i, part, out)
    return out.astype(BF16)


def key_rows(k_t, bias):
    keys = k_t.shape[1]
    aux = rows16([bias, -1.0, -1.0, -1.0], keys)
    pad = jnp.zeros((48, keys), BF16)
    return jnp.concatenate([k_t, k_t, aux, pad], axis=0).T


def fwd_kernel(heads, q_block, chunk, q_ref, k_ref, v_ref, bias_ref, o_ref, l_ref, k_aug, s_a, s_b):
    queries, keys = q_ref.shape[1], k_ref.shape[1]
    steps = [(h, b) for h in range(heads) for b in range(queries // q_block)]
    slots = (s_a, s_b)
    ones = rows16([1.0], keys)

    def scores(step):
        h, b = steps[step]
        slot = slots[step % 2]
        rows = slice(h * HEAD, (h + 1) * HEAD)
        if b == 0:
            k_aug[h % 2] = key_rows(k_ref[rows, :], bias_ref[...])
        hi, lo = scaled_pair(q_ref[rows, b * q_block:(b + 1) * q_block])
        q_aug = jnp.concatenate(
            [hi, lo, rows16([1.0], q_block), jnp.zeros((48, q_block), BF16)], axis=0)
        top = None
        for c in range(keys // chunk):
            s = jnp.dot(k_aug[h % 2, c * chunk:(c + 1) * chunk, :], q_aug, preferred_element_type=F32)
            slot[c * chunk:(c + 1) * chunk, :] = s
            m = jnp.max(s, axis=0, keepdims=True)
            top = m if top is None else jnp.maximum(top, m)
        return top

    def mix(step, top):
        h, b = steps[step]
        slot = slots[step % 2]
        rows = slice(h * HEAD, (h + 1) * HEAD)
        cols = slice(b * q_block, (b + 1) * q_block)
        v_aug = jnp.concatenate([v_ref[rows, :], ones], axis=0)
        acc = jnp.zeros((48, q_block), F32)
        for c in range(keys // chunk):
            p = jnp.exp2(slot[c * chunk:(c + 1) * chunk, :] - top).astype(BF16)
            acc = acc + jnp.dot(v_aug[:, c * chunk:(c + 1) * chunk], p, preferred_element_type=F32)
        total = acc[HEAD:HEAD + 1, :]
        o_ref[rows, cols] = (acc[:HEAD] * (1.0 / total)).astype(BF16)
        l_ref[0, h:h + 1, cols] = top + jnp.log2(total)

    top = scores(0)
    for step in range(len(steps)):
        after = scores(step + 1) if step + 1 < len(steps) else None
        mix(step, top)
        top = after


def attention_forward(q_t, k_t, v_t, bias, heads=2, q_block=256, chunk=512):
    width, queries = q_t.shape
    keys = k_t.shape[1]
    all_heads = width // HEAD
    rows = heads * HEAD
    return pl.pallas_call(
        functools.partial(fwd_kernel, heads, q_block, chunk),
        name="attn_fwd",
        grid=(all_heads // heads,),
        out_shape=(jax.ShapeDtypeStruct((width, queries), BF16),
                   jax.ShapeDtypeStruct((all_heads // heads, heads, queries), F32)),
        in_specs=[pl.BlockSpec((rows, queries), lambda i: (i, 0)),
                  pl.BlockSpec((rows, keys), lambda i: (i, 0)),
                  pl.BlockSpec((rows, keys), lambda i: (i, 0)),
                  pl.BlockSpec((1, keys), lambda i: (0, 0))],
        out_specs=(pl.BlockSpec((rows, queries), lambda i: (i, 0)),
                   pl.BlockSpec((1, heads, queries), lambda i: (i, 0, 0))),
        scratch_shapes=[pltpu.VMEM((2, keys, 128), BF16),
                        pltpu.VMEM((keys, q_block), F32),
                        pltpu.VMEM((keys, q_block), F32)],
        compiler_params=pltpu.CompilerParams(vmem_limit_bytes=56 << 20),
        cost_estimate=pl.CostEstimate(
            flops=16 * 2 * HEAD * 2 * all_heads * queries * keys,
            transcendentals=all_heads * queries * keys,
            bytes_accessed=4 * width * keys * 2),
    )(q_t, k_t, v_t, bias)


def bwd_kernel(heads, q_block, chunk, last, *refs):
    q_ref, k_ref, v_ref, bias_ref, o_ref, g_ref, l_ref = refs[:7]
    carried_ref = refs[7] if last else None
    dq_ref, dk_ref, dv_ref, k_aug, v_aug, dk_acc, dv_acc = refs[7 + last:]
    queries, keys = q_ref.shape[1], k_ref.shape[1]
    scale = 1.0 / math.sqrt(HEAD)
    nt = (((1,), (1,)), ((), ()))
    for h in range(heads):
        rows = slice(h * HEAD, (h + 1) * HEAD)
        k_t = k_ref[rows, :]
        k_aug[h % 2] = key_rows(k_t, bias_ref[...])
        minus = rows16([-1.0, -1.0, -1.0], keys)
        v_aug[h % 2] = jnp.concatenate(
            [v_ref[rows, :], minus, jnp.zeros((80, keys), BF16)], axis=0).T
        for b in range(queries // q_block):
            cols = slice(b * q_block, (b + 1) * q_block)
            q_t = q_ref[rows, cols]
            g_t = g_ref[rows, cols]
            hi, lo = scaled_pair(q_t)
            l3 = three_terms(l_ref[0, h:h + 1, cols])
            q_aug = jnp.concatenate(
                [hi, lo, rows16([1.0] + [t.astype(F32) for t in l3], q_block),
                 jnp.zeros((48, q_block), BF16)], axis=0)
            inner = jnp.sum(g_t.astype(F32) * o_ref[rows, cols].astype(F32), axis=0, keepdims=True)
            g_aug = jnp.concatenate(
                [g_t, rows16([t.astype(F32) for t in three_terms(inner)], q_block),
                 jnp.zeros((80, q_block), BF16)], axis=0)
            dq = jnp.zeros((HEAD, q_block), F32)
            for c in range(keys // chunk):
                span = slice(c * chunk, (c + 1) * chunk)
                p = jnp.exp2(jnp.dot(k_aug[h % 2, span, :], q_aug, preferred_element_type=F32))
                d = p * jnp.dot(v_aug[h % 2, span, :], g_aug, preferred_element_type=F32)
                p, d = p.astype(BF16), d.astype(BF16)
                dv = lax.dot_general(g_t, p, nt, preferred_element_type=F32)
                dk = lax.dot_general(q_t, d, nt, preferred_element_type=F32)
                if b == 0:
                    dv_acc[h % 2, :, span] = dv
                    dk_acc[h % 2, :, span] = dk
                else:
                    dv_acc[h % 2, :, span] += dv
                    dk_acc[h % 2, :, span] += dk
                dq = dq + jnp.dot(k_t[:, span], d, preferred_element_type=F32)
            if last:
                dq_ref[rows, cols] = ((carried_ref[rows, cols] + dq) * scale).astype(BF16)
            else:
                dq_ref[rows, cols] = dq
        dv_ref[rows, :] = dv_acc[h % 2].astype(BF16)
        dk_ref[rows, :] = (dk_acc[h % 2] * scale).astype(BF16)


def attention_backward(q_t, k_t, v_t, bias, o_t, g_t, lse, part, carried=None,
                       heads=2, q_block=512, chunk=512):
    width, queries = q_t.shape
    keys = k_t.shape[1] // 2
    rows = heads * HEAD
    last = carried is not None
    q_spec = pl.BlockSpec((rows, queries), lambda i: (i, 0))
    k_spec = pl.BlockSpec((rows, keys), lambda i: (i, part))
    out = pl.BlockSpec((rows, keys), lambda i: (i, 0))
    return pl.pallas_call(
        functools.partial(bwd_kernel, heads, q_block, chunk, last),
        name="attn_bwd_last" if last else "attn_bwd_first",
        grid=(width // rows,),
        out_shape=(jax.ShapeDtypeStruct((width, queries), BF16 if last else F32),
                   jax.ShapeDtypeStruct((width, keys), BF16),
                   jax.ShapeDtypeStruct((width, keys), BF16)),
        in_specs=[q_spec, k_spec, k_spec, pl.BlockSpec((1, keys), lambda i: (0, part)), q_spec, q_spec,
                  pl.BlockSpec((1, heads, queries), lambda i: (i, 0, 0))] + [q_spec] * last,
        out_specs=(q_spec, out, out),
        scratch_shapes=[pltpu.VMEM((2, keys, 128), BF16), pltpu.VMEM((2, keys, 128), BF16),
                        pltpu.VMEM((2, HEAD, keys), F32), pltpu.VMEM((2, HEAD, keys), F32)],
        compiler_params=pltpu.CompilerParams(vmem_limit_bytes=56 << 20),
        cost_estimate=pl.CostEstimate(
            flops=8 * 5 * 2 * width * queries * keys,
            transcendentals=width // HEAD * queries * keys,
            bytes_accessed=width * (5 * queries + 4 * keys) * 2),
    )(q_t, k_t, v_t, bias, o_t, g_t, lse, *([carried] if last else []))

TN = (((0,), (0,)), ((), ()))
NT = (((1,), (1,)), ((), ()))


def dot32(a, b, dims=(((1,), (0,)), ((), ()))):
    return lax.dot_general(a, b, dims, preferred_element_type=F32)


def gelu_parts(u):
    x = jnp.abs(u) * math.sqrt(0.5)
    t = 1.0 / (1.0 + 0.3275911 * x)
    e = jnp.exp(-0.5 * u * u)
    poly = t * (0.254829592 + t * (-0.284496736 + t * (1.421413741 + t * (-1.453152027 + t * 1.061405429))))
    tail = 0.5 * poly * e
    cdf = jnp.where(u < 0, tail, 1.0 - tail)
    return u * cdf, cdf + u * e * (1.0 / math.sqrt(2.0 * math.pi))


def ffn_kernel(chained, *refs):
    n_ref, g_ref, wu_ref, bu_ref, wd_ref = refs[:5]
    f_ref, dn_ref, gu_ref, gd_ref, gb_ref = refs[5 + 2 * chained:]
    first = pl.program_id(0) == 0
    wu, wd, n, dy = wu_ref[...], wd_ref[...], n_ref[...], g_ref[...]
    value, slope = gelu_parts(dot32(n, wu) + bu_ref[0])
    value = value.astype(BF16)
    du = (dot32(dy, wd, NT) * slope).astype(BF16)
    gb_ref[0] = jnp.sum(du.astype(F32), axis=0, keepdims=True)
    gu_ref[...] = dot32(n, du, TN).astype(gu_ref.dtype)
    gd_ref[...] = dot32(value, dy, TN).astype(gd_ref.dtype)
    f, dn = dot32(value, wd), dot32(du, wu, NT)

    @pl.when(first)
    def _():
        f_ref[...] = refs[5][...] + f if chained else f
        dn_ref[...] = refs[6][...] + dn if chained else dn

    @pl.when(jnp.logical_not(first))
    def _():
        f_ref[...] += f
        dn_ref[...] += dn


def feed_forward(normed, grad, w_up, up_bias, w_down, carried, held, block=640):
    tokens, width = normed.shape
    units = w_up.shape[1]
    chained = carried is not None
    whole = pl.BlockSpec((tokens, width), lambda i: (0, 0), pipeline_mode=pl.Buffered(1))
    total = pl.BlockSpec((tokens, width), lambda i: (0, 0))
    bias = pl.BlockSpec((1, 1, block), lambda i: (i, 0, 0))
    up = pl.BlockSpec((width, block), lambda i: (0, i))
    down = pl.BlockSpec((block, width), lambda i: (i, 0))
    f, dn, gu, gd, gb = pl.pallas_call(
        functools.partial(ffn_kernel, chained),
        name="ffn",
        grid=(units // block,),
        out_shape=(jax.ShapeDtypeStruct((tokens, width), F32),
                   jax.ShapeDtypeStruct((tokens, width), F32),
                   jax.ShapeDtypeStruct((width, units), held),
                   jax.ShapeDtypeStruct((units, width), held),
                   jax.ShapeDtypeStruct((units // block, 1, block), F32)),
        in_specs=[whole, whole, up, bias, down] + [whole, whole] * chained,
        out_specs=(total, total, up, down, bias),
        input_output_aliases={5: 0, 6: 1} if chained else {},
        compiler_params=pltpu.CompilerParams(vmem_limit_bytes=56 << 20),
        cost_estimate=pl.CostEstimate(
            flops=24 * tokens * width * units, transcendentals=tokens * units * 2,
            bytes_accessed=units * width * 12 + tokens * width * 20),
    )(normed, grad, w_up, up_bias.reshape(units // block, 1, block), w_down, *(carried or ()))
    return (f, dn), gu, gd, gb.reshape(units)


epsilon = 1e-05
masked_score = -1000000000.0


def layer_norm(inputs, gain_vec, bias_vec):
    center = inputs - jnp.mean(inputs, axis=-1, keepdims=True)
    spread = jnp.mean(center * center, axis=-1, keepdims=True)
    return center * lax.rsqrt(spread + epsilon) * gain_vec + bias_vec


def gelu_exact(inputs):
    return jax.nn.gelu(inputs, approximate=False)


def pair_keys(offsets, item_lengths, key_flags):
    seq_len = key_flags.shape[1]
    column = lax.broadcasted_iota(jnp.int32, (2, seq_len), 1)
    second = lax.broadcasted_iota(jnp.int32, (2, seq_len), 0) == 1
    joined = offsets[1] > offsets[0]
    repeat = second & joined & (offsets[1] + column < offsets[0] + seq_len)
    live_keys = (key_flags == 1) & (column < item_lengths[:, None]) & jnp.logical_not(repeat)
    return live_keys, joined


def einsum32(spec, a, b):
    return jnp.einsum(spec, a, b, preferred_element_type=F32)


def body(
    dp_count,
    tokens,
    window_offsets,
    lengths,
    key_mask,
    ln1_gain,
    ln1_bias,
    w_qkv,
    qv_bias,
    w_out,
    out_bias,
    ln2_gain,
    ln2_bias,
    w_up,
    up_bias,
    w_down,
    down_bias,
    out_grad,
):
    side = lax.axis_index("tensor")
    core = lax.axis_index("dp") % 2

    def swap_side(x):
        return lax.ppermute(x, "tensor", [(0, 1), (1, 0)])

    def swap_core(x):
        return lax.ppermute(x, "dp", [(i, i ^ 1) for i in range(dp_count)])

    def halves(x, axis):
        size = x.shape[axis] // 2
        return (lax.dynamic_slice_in_dim(x, core * size, size, axis),
                lax.dynamic_slice_in_dim(x, (1 - core) * size, size, axis))

    def ordered(first, second, flag, axis):
        return jnp.where(flag == 0, jnp.concatenate([first, second], axis),
                         jnp.concatenate([second, first], axis))

    def gathered(near):
        other_near = swap_side(near)
        return other_near, swap_core(other_near)

    def summed(x):
        for bit in range(dp_count.bit_length() - 1):
            x = x + lax.ppermute(x, "dp", [(i, i ^ (1 << bit)) for i in range(dp_count)])
        return x + swap_side(x)

    def core_sum(mine, kind):
        groups = [list(range(c, dp_count, 2)) for c in range(2)]
        groups = (groups, groups[::-1], [g[::-1] for g in groups])[kind]
        return lax.psum(mine, "dp", axis_index_groups=groups)

    def total(mine, axis):
        return ordered(mine, swap_core(mine), core, axis).astype(F32)

    def met(near, other_near, far, other_far):
        got, got_other = swap_core(far), swap_core(other_far)
        crossing = (other_near.astype(F32) + got_other.astype(F32)).astype(BF16)
        return near, got, swap_side(crossing), crossing

    def joined_sum(near, got, across):
        return (near.astype(F32) + got.astype(F32) + across.astype(F32)).astype(BF16)

    seq_len, width = tokens.shape
    local = qv_bias.shape[1]
    qkv_near, qkv_far = halves(w_qkv, 2)
    w_qkv_all = jnp.concatenate((qkv_near, qkv_far) + gathered(qkv_near), 2)
    biases = jnp.concatenate([qv_bias.reshape(-1), up_bias])
    biases_other = swap_side(biases)
    tokens_other = swap_side(tokens)
    qv_all = jnp.concatenate(
        halves(qv_bias, 1) + halves(biases_other[:2 * local].reshape(2, local), 1), 1)
    up_bias_parts = halves(up_bias, 0) + halves(biases_other[2 * local:], 0)
    out_near, out_far = halves(w_out, 0)
    up_near, up_far = halves(w_up, 1)
    down_near, down_far = halves(w_down, 0)
    tokens_other, out_near, up_near, down_near = lax.optimization_barrier(
        (tokens_other, out_near, up_near, down_near))
    w_out_all = jnp.concatenate((out_near, out_far) + gathered(out_near), 0)
    w_up_parts = (up_near, up_far) + gathered(up_near)
    w_down_parts = (down_near, down_far) + gathered(down_near)

    live, joined = pair_keys(window_offsets, lengths, key_mask)
    live_own = lax.dynamic_index_in_dim(live, side, 0, keepdims=False)
    live_other = lax.dynamic_index_in_dim(live, 1 - side, 0, keepdims=False) & joined
    bias = jnp.where(jnp.concatenate([live_own, live_other]), 0.0, masked_score)[None].astype(F32)

    tokens_f = tokens.astype(F32)
    normed = layer_norm(tokens_f, ln1_gain, ln1_bias).astype(BF16)
    normed_other = layer_norm(tokens_other.astype(F32), ln1_gain, ln1_bias).astype(BF16)
    normed_both = jnp.concatenate([normed, normed_other], axis=0)
    query = (einsum32("td,de->et", normed, w_qkv_all[0]) + qv_all[0][:, None]).astype(BF16)
    key = einsum32("td,de->et", normed_both, w_qkv_all[1]).astype(BF16)
    value = (einsum32("td,de->et", normed_both, w_qkv_all[2]) + qv_all[1][:, None]).astype(BF16)
    heads_out, log_norm = attention_forward(query, key, value, bias)

    residual_mid = tokens_f + (einsum32("et,ed->td", heads_out, w_out_all) + out_bias)
    normed_mid = layer_norm(residual_mid, ln2_gain, ln2_bias).astype(BF16)
    carried, grads = None, {}
    for part in (1, 3, 2, 0):
        carried, grad_up, grad_down, grad_bias = feed_forward(
            normed_mid, out_grad, w_up_parts[part], up_bias_parts[part], w_down_parts[part],
            carried, BF16 if part in (1, 3) else F32)
        grads[part] = (grad_up, grad_down, grad_bias)
    branch, grad_normed_mid = carried
    layer_out = (residual_mid + (branch + down_bias)).astype(BF16)
    up_sums = met(*(grads[part][0] for part in (0, 2, 1, 3)))
    down_sums = met(*(grads[part][1] for part in (0, 2, 1, 3)))
    grad_up_bias = [grads[part][2] for part in range(4)]
    _, norm2_back = jax.vjp(layer_norm, residual_mid, ln2_gain, ln2_bias)
    grad_mid_part, grad_ln2_gain, grad_ln2_bias = norm2_back(grad_normed_mid)
    grad_mid = out_grad.astype(F32) + grad_mid_part
    grad_mid_low = grad_mid.astype(BF16)
    grad_heads = einsum32("td,ed->et", grad_mid_low, w_out_all).astype(BF16)
    grad_heads, crossing_up, crossing_down = lax.optimization_barrier(
        (grad_heads, up_sums[3], down_sums[3]))
    grad_w_out = einsum32("et,td->ed", heads_out, grad_mid_low)
    grad_down_bias = jnp.sum(out_grad, axis=0, dtype=F32)
    grad_out_bias = jnp.sum(grad_mid_low, axis=0, dtype=F32)

    query_part, other_grad_key, other_grad_value = attention_backward(
        query, key, value, bias, heads_out, grad_heads, log_norm, 1)
    to_other = (einsum32("et,de->td", other_grad_key, w_qkv_all[1])
                + einsum32("et,de->td", other_grad_value, w_qkv_all[2])).astype(BF16)
    other_parts = [einsum32("et,td->ed", x, normed_other) for x in (other_grad_key, other_grad_value)]
    other_value_sum = jnp.sum(other_grad_value, axis=1, dtype=F32)
    mine_up = joined_sum(*up_sums[:3])
    mine_down = joined_sum(*down_sums[:3])
    query_part, mine_up, mine_down, to_other, other_parts, other_value_sum = lax.optimization_barrier(
        (query_part, mine_up, mine_down, to_other, other_parts, other_value_sum))
    from_other = swap_side(to_other)
    mine_up, mine_down = core_sum(mine_up, 0), core_sum(mine_down, 1)
    grad_query, grad_key, grad_value = attention_backward(
        query, key, value, bias, heads_out, grad_heads, log_norm, 0, query_part)
    grad_query, from_other = lax.optimization_barrier((grad_query, from_other))

    grad_proj = jnp.stack([
        grad_w_out,
        einsum32("et,td->ed", grad_query, normed),
        einsum32("et,td->ed", grad_key, normed) + other_parts[0],
        einsum32("et,td->ed", grad_value, normed) + other_parts[1]])
    near, far, other_near, other_far = jnp.split(grad_proj, 4, axis=1)
    mine_proj = joined_sum(*met(near, other_near, far.astype(BF16), other_far.astype(BF16))[:3])
    mine_proj, mine_up, mine_down = lax.optimization_barrier((mine_proj, mine_up, mine_down))
    grad_w_up, grad_w_down = total(mine_up, 1), total(mine_down, 0)
    grad_proj = total(core_sum(mine_proj, 2), 1)
    grad_w_out = grad_proj[0]
    grad_w_qkv = grad_proj[1:].swapaxes(1, 2)

    grad_normed = (einsum32("et,de->td", grad_query, w_qkv_all[0])
                   + einsum32("et,de->td", grad_key, w_qkv_all[1])
                   + einsum32("et,de->td", grad_value, w_qkv_all[2]) + from_other.astype(F32))
    _, norm1_back = jax.vjp(layer_norm, tokens_f, ln1_gain, ln1_bias)
    grad_tok_part, grad_ln1_gain, grad_ln1_bias = norm1_back(grad_normed)
    tokens_grad = (grad_mid + grad_tok_part).astype(BF16)

    def global_order(x):
        near, far, other_near, other_far = jnp.split(x, 4, axis=-1)
        return ordered(ordered(near, far, core, -1), ordered(other_near, other_far, core, -1), side, -1)

    value_sum = jnp.sum(grad_value, axis=1, dtype=F32) + other_value_sum
    qv_sums = global_order(jnp.stack([jnp.sum(grad_query, axis=1, dtype=F32), value_sum]))
    near, far, other_near, other_far = grad_up_bias
    up_sum = ordered(ordered(near, far, core, 0), ordered(other_near, other_far, core, 0), side, 0)
    small = summed(jnp.concatenate([
        jnp.stack([grad_ln1_gain, grad_ln1_bias, grad_ln2_gain, grad_ln2_bias,
                   grad_out_bias, grad_down_bias]), qv_sums, up_sum.reshape(-1, width)]))
    grad_qv_bias = lax.dynamic_slice_in_dim(small[6:8], side * local, local, 1)
    grad_up_bias = lax.dynamic_slice_in_dim(
        small[8:].reshape(-1), side * up_bias.shape[0], up_bias.shape[0], 0)
    vectors = [small[i] for i in range(6)]
    return (
        layer_out,
        tokens_grad,
        vectors[0],
        vectors[1],
        grad_w_qkv,
        grad_qv_bias,
        grad_w_out,
        vectors[4],
        vectors[2],
        vectors[3],
        grad_w_up,
        grad_up_bias,
        grad_w_down,
        vectors[5],
    )


def solution(mesh):
    in_specs = (
        P(("dp", "tensor"), None),
        P("dp"),
        P("dp"),
        P("dp", None),
        P(),
        P(),
        P(None, None, "tensor"),
        P(None, "tensor"),
        P("tensor", None),
        P(),
        P(),
        P(),
        P(None, "tensor"),
        P("tensor"),
        P("tensor", None),
        P(),
        P(("dp", "tensor"), None),
    )
    out_specs = (
        P(("dp", "tensor"), None),
        P(("dp", "tensor"), None),
        P(),
        P(),
        P(None, None, "tensor"),
        P(None, "tensor"),
        P("tensor", None),
        P(),
        P(),
        P(),
        P(None, "tensor"),
        P("tensor"),
        P("tensor", None),
        P(),
    )
    bound = functools.partial(body, mesh.shape["dp"])
    return jax.shard_map(bound, mesh=mesh, in_specs=in_specs, out_specs=out_specs, check_vma=False)
```
